256 devices in a mesh: gx: 32 (over z, y_hi, core), gy: 8 (over y_lo, x).
Axes of the slice: x: 4, y: 4 (y_hi: 2, y_lo: 2; y = y_hi * 2 + y_lo), z: 8, core: 2. Of those that a mesh axis runs over, the one named last changes fastest.
Arguments:
- prognostic_values: float32 [3, 6, 4096, 4096], P(None, None, 'gx', 'gy'), may hold values from -6 to 6
- forcing_host_values: bfloat16 [3, 6, 4096, 4096], P(None, None, 'gx', 'gy'), may hold values from -6 to 6
- strength: float32 [3, 6], replicated, may hold values from 50 to 200
- level_height: float32 [3], replicated, may hold values from 0.2 to 3
- pbl_height: float32 [4096, 4096], P('gx', 'gy'), may hold values from 0.2 to 3
Outputs:
- tendency: bfloat16 [3, 6, 4096, 4096], P(None, None, 'gx', 'gy')
- energy: float32 [3, 6], replicated
The draws below stay inside these ranges and needn't reach their ends.
All inputs are finite; a program needn't handle non-finite values.
Results may differ from the reference program's by a relative error of at most 0.001.
Values sent between devices are 32-bit elements; how exact they have to be, the bound alone decides.
A program may use at most 64 MiB of HBM per device.

```python
import math
import jax
import jax.numpy as jnp
from jax import lax

KX = 32
KY = 32
VARS = 6
LEV = 3
NX = 4096
NY = 4096


def level_of(rng, extent, cuts, low, high):
    def one(dim, shards_of):
        steps = jax.random.uniform(jax.random.fold_in(jax.random.fold_in(rng, 6), dim), (shards_of,), jnp.float32, low / len(cuts), high / len(cuts))
        return jnp.repeat(jnp.exp(steps), extent[dim] // shards_of).reshape((-1,) + (1,) * (len(extent) - dim - 1))

    gain = one(*cuts[0])
    for cut in cuts[1:]:
        gain = gain * one(*cut)
    return gain


def gaussian(own_key, extent, deviation, most, shards=(), dtype=jnp.bfloat16):
    level = level_of(own_key, extent, shards, -0.22, 0.18) if shards else 1.0
    values = jax.random.normal(own_key, extent, jnp.float32) * deviation * level
    return jnp.minimum(jnp.maximum(values, -most), most).astype(dtype)


def setup_inputs(seed: int = 0) -> dict:
    seeds = jax.random.split(jax.random.key(seed), 6)
    prognostic_values = gaussian(seeds[0], (LEV, VARS, NX, NY), 1.0, 6.0, ((2, 32), (3, 8)), jnp.float32)
    forcing_host_values = gaussian(seeds[1], (LEV, VARS, NX, NY), 1.0, 6.0, ((2, 32), (3, 8)))
    strength = jnp.clip(jnp.exp(jax.random.uniform(seeds[2], (LEV, VARS), jnp.float32, math.log(50.0), math.log(200.0))), 50.0, 200.0)
    level_height = jnp.clip(jax.random.uniform(seeds[3], (LEV,), jnp.float32, 0.2, 3.0), 0.2, 3.0)
    pbl_height = jnp.clip(0.2 + 2.8 * jax.random.uniform(seeds[4], (NX, NY), jnp.float32) ** level_of(seeds[4], (NX, NY), ((0, 32), (1, 8)), -0.2, 0.2), 0.2, 3.0)
    return {"prognostic_values": prognostic_values, "forcing_host_values": forcing_host_values, "strength": strength, "level_height": level_height, "pbl_height": pbl_height}


ramp_depth = 0.25

def cosine_table(total, modes, start, count):
    index = (start + jnp.arange(count)).astype(jnp.float32)
    waves = jnp.arange(modes).astype(jnp.float32)
    scales = jnp.where(waves == 0.0, jnp.sqrt(1.0 / total), jnp.sqrt(2.0 / total)).astype(jnp.float32)
    return scales[None, :] * jnp.cos(jnp.pi * (index[:, None] + 0.5) * waves[None, :] / total)

def reference(prognostic_values, forcing_host_values, strength, level_height, pbl_height):
    meridional_cosines = cosine_table(NX, KX, 0, NX)
    col_basis = cosine_table(NY, KY, 0, NY)
    largest_wavenumber = lax.Precision.HIGHEST

    def one_level(items):
        model, driver, gains, altitude_factor = items
        diff = driver.astype(jnp.float32) - model
        part = jnp.einsum('vij,jb->vib', diff, col_basis, precision=largest_wavenumber)
        mode_factors = jnp.einsum('wl,ywg->ylg', meridional_cosines, part, precision=largest_wavenumber)
        restored_fields = jnp.einsum('ky,jyp->jkp', meridional_cosines, mode_factors, precision=largest_wavenumber)
        recon = jnp.einsum('vib,jb->vij', restored_fields, col_basis, precision=largest_wavenumber)
        damping_share = 1.0 / (1.0 + jnp.exp(-(altitude_factor - pbl_height) / ramp_depth))
        tend = (gains[:, None, None] * damping_share[None] * recon).astype(jnp.bfloat16)
        energy = lax.optimization_barrier(jnp.sum(recon * recon, axis=(1, 2))) / (KX * KY)
        return (tend, energy)
    tendency, energy = lax.map(one_level, (prognostic_values, forcing_host_values, strength, level_height))
    return (tendency, energy)
```

```python
import functools

import jax
import jax.numpy as jnp
from jax import lax
from jax.experimental import pallas as pl
from jax.experimental.pallas import tpu as pltpu
from jax.sharding import PartitionSpec as P

MODES = 32
FIELDS = 18
VARS = 6
LEVELS = 3
GROUPS = 5
ROWS = 128
COLS = 512
PLANES = 8
PLANE = 32
ramp_depth = 0.25
f32 = jnp.float32
bf16 = jnp.bfloat16


def fields_of(group):
    return range(4 * group, min(4 * group + 4, FIELDS))


def owner_of(group, block):
    x, y = block, (block + group) % 4
    core = 0 if group == 0 else 1
    return (y // 2) * 2 + core, (y % 2) * 4 + x


def cosines(position, mode, total):
    turn = ((2 * position + 1) * mode) & (4 * total - 1)
    turn = jnp.minimum(turn, 4 * total - turn)
    back = turn > total
    turn = jnp.where(back, 2 * total - turn, turn)
    steep = 2 * turn > total
    angle = jnp.where(steep, total - turn, turn).astype(f32) * (jnp.pi / (2 * total))
    square = angle * angle
    even = 1.0 + square * (-0.5 + square * (1 / 24 + square * (-1 / 720 + square * (1 / 40320))))
    odd = angle * (1.0 + square * (-1 / 6 + square * (1 / 120 + square * (-1 / 5040 + square * (1 / 362880)))))
    value = jnp.where(steep, odd, even)
    value = jnp.where(back, -value, value)
    scale = jnp.where(mode == 0, (1.0 / total) ** 0.5, (2.0 / total) ** 0.5).astype(f32)
    return scale * value


def split(value):
    high = value.astype(bf16)
    return high, (value - high.astype(f32)).astype(bf16)


def iota(shape, dim):
    return lax.broadcasted_iota(jnp.int32, shape, dim)


def kernel(
    prog_hbm, forc_hbm, strength, height, pbl_hbm, out, energy_ref,
    prog, forc, pbl, weight, first_table, row_left, row_right, last_table,
    part, planes_in, totals_in, coefs,
    prog_sem, forc_sem, pbl_sem, sent1, got1, sent2, got2, sent3, got3,
):
    gx, gy = lax.axis_index("gx"), lax.axis_index("gy")
    z, place = gx // 4, gx % 4
    core, x = place % 2, gy % 4
    y = (place // 2) * 2 + gy // 4
    mine = place * 8 + gy
    lag = (y - x + 4) % 4
    group_own = jnp.where(core == 0, 0, jnp.where(lag == 0, 4, lag))
    owner = (core == 1) | (lag == 0)

    def loads(f):
        l, v = divmod(f, VARS)
        return (
            pltpu.make_async_copy(prog_hbm.at[l, v], prog.at[f], prog_sem.at[f]),
            pltpu.make_async_copy(forc_hbm.at[l, v], forc.at[f], forc_sem.at[f]),
        )

    for f in range(FIELDS):
        for copy in loads(f):
            copy.start()
    load_pbl = pltpu.make_async_copy(pbl_hbm, pbl, pbl_sem)
    load_pbl.start()

    barrier = pltpu.get_barrier_semaphore()

    def greet_plane(k, _):
        peer = (mine + k) % PLANE
        pl.semaphore_signal(
            barrier, inc=1, device_id={"gx": z * 4 + peer // 8, "gy": peer % 8},
            device_id_type=pl.DeviceIdType.MESH,
        )
        return _

    def greet_planes(k, _):
        pl.semaphore_signal(
            barrier, inc=1, device_id={"gx": ((z + k) % PLANES) * 4 + place, "gy": gy},
            device_id_type=pl.DeviceIdType.MESH,
        )
        return _

    lax.fori_loop(1, PLANE, greet_plane, 0)
    lax.fori_loop(1, PLANES, greet_planes, 0)

    for piece in range(4):
        rows = pl.ds(piece * 128, 128)
        table = cosines(gy * COLS + piece * 128 + iota((128, 128), 0), iota((128, 128), 1) % MODES, 4096)
        high, low = split(table)
        first_table[rows, 0:128] = high
        first_table[rows, 128:256] = low
        table = cosines(gy * COLS + piece * 128 + iota((128, 128), 1), iota((128, 128), 0) % MODES, 4096)
        high, low = split(table)
        last_table[:, piece * 128 : piece * 128 + 128] = jnp.where(iota((128, 128), 0) < 64, high.astype(f32), low.astype(f32)).astype(bf16)
    table = cosines(gx * ROWS + iota((32, 128), 1), iota((32, 128), 0), 4096)
    high, low = split(table)
    row_left[...] = jnp.concatenate([high, high, low, low], axis=1)
    table = cosines(gx * ROWS + iota((128, 128), 0), iota((128, 128), 1) % MODES, 4096)
    high, low = split(table)
    row_right[...] = jnp.where(iota((128, 128), 1) < 64, high.astype(f32), low.astype(f32)).astype(bf16)

    lane_block = iota((ROWS, 128), 1) // MODES

    def forward(group):
        packed = jnp.zeros((ROWS, 128), f32)
        for q, f in enumerate(fields_of(group)):
            for copy in loads(f):
                copy.wait()
            diff = forc[f].astype(f32) - prog[f]
            high, low = split(diff)
            both = jnp.dot(high, first_table[...], preferred_element_type=f32) + jnp.dot(
                low, first_table[...], preferred_element_type=f32
            )
            packed = jnp.where(lane_block == q, both[:, :128] + both[:, 128:], packed)
        high, low = split(packed)
        stacked = jnp.concatenate([high, low, high, low], axis=0)
        result = jnp.dot(row_left[...], stacked, preferred_element_type=f32)
        for block in range(4):
            part[group, block] = result[block * 8 : block * 8 + 8]

    def send_parts(group):
        for block in range(4):
            to_place, to_gy = owner_of(group, block)
            @pl.when(mine != to_place * 8 + to_gy)
            def _():
                pltpu.make_async_remote_copy(
                    part.at[group, block], planes_in.at[mine], sent1, got1,
                    device_id={"gx": z * 4 + to_place, "gy": to_gy}, device_id_type=pl.DeviceIdType.MESH,
                ).start()

    for group in range(GROUPS):
        forward(group)
        if group == 0:
            pl.semaphore_wait(barrier, PLANE - 1 + PLANES - 1)
        send_parts(group)

    load_pbl.wait()
    for l in range(LEVELS):
        weight[l] = 1.0 / (1.0 + jnp.exp(-(height[l] - pbl[...]) / ramp_depth))

    def arrived(ref, count, sem):
        whole = ref.at[pl.ds(0, count)]
        pltpu.make_async_copy(whole, whole, sem).wait()

    unit_own = group_own * 4 + x

    @pl.when(owner)
    def _():
        planes_in[mine] = part[group_own, x]
        arrived(planes_in, PLANE - 1, got1)
        sums = [planes_in[k] for k in range(PLANE)]
        while len(sums) > 1:
            sums = [a + b for a, b in zip(sums[::2], sums[1::2])]
        totals_in[z] = sums[0]
        for k in range(1, PLANES):
            pltpu.make_async_remote_copy(
                totals_in.at[z], totals_in.at[z], sent2, got2,
                device_id={"gx": ((z + k) % PLANES) * 4 + place, "gy": gy}, device_id_type=pl.DeviceIdType.MESH,
            ).start()
        arrived(totals_in, PLANES - 1, got2)
        sums = [totals_in[k] for k in range(PLANES)]
        while len(sums) > 1:
            sums = [a + b for a, b in zip(sums[::2], sums[1::2])]
        coefs[unit_own] = sums[0]

        def send_total(k, _):
            peer = (mine + k) % PLANE
            pltpu.make_async_remote_copy(
                coefs.at[unit_own], coefs.at[unit_own], sent3, got3.at[group_own],
                device_id={"gx": z * 4 + peer // 8, "gy": peer % 8}, device_id_type=pl.DeviceIdType.MESH,
            ).start()
            return _

        lax.fori_loop(1, PLANE, send_total, 0)

    spot_row, spot_col = iota((LEVELS, VARS), 0), iota((LEVELS, VARS), 1)
    block_lanes = iota((MODES, 128), 1) // MODES
    energies = jnp.zeros((LEVELS, VARS), f32)
    for group in range(GROUPS):
        holds = owner & (group_own == group)

        @pl.when(holds)
        def _():
            arrived(coefs, 3, got3.at[group])

        @pl.when(jnp.logical_not(holds))
        def _():
            arrived(coefs, 4, got3.at[group])

        coef = jnp.concatenate([coefs[4 * group + block] for block in range(4)], axis=0)
        for q, f in enumerate(fields_of(group)):
            l, v = divmod(f, VARS)
            only = jnp.where(block_lanes == q, coef, 0.0)
            total = jnp.sum(only * only, axis=(0, 1), keepdims=True) * (1.0 / (MODES * MODES))
            energies = jnp.where((spot_row == l) & (spot_col == v), total, energies)
            four = only + pltpu.roll(only, 64, 1)
            four = four + pltpu.roll(four, 32, 1)
            high, low = split(four)
            stacked = jnp.concatenate([high, low, high, low], axis=0)
            along = jnp.dot(row_right[...], stacked, preferred_element_type=f32)
            high, low = split(along)
            left = jnp.where(lane_block % 2 == 0, high.astype(f32), low.astype(f32)).astype(bf16)
            recon = jnp.dot(left, last_table[...], preferred_element_type=f32)
            out[l, v] = ((strength[l, v] * weight[l]) * recon).astype(bf16)
    energy_ref[...] = energies

    @pl.when(owner)
    def _():
        flat = pltpu.make_async_copy(part.at[pl.ds(0, 4)], part.at[pl.ds(0, 4)], sent1)
        flat.wait()
        rest = part.at[4, pl.ds(0, 3)]
        pltpu.make_async_copy(rest, rest, sent1).wait()
        arrived(totals_in, PLANES - 1, sent2)
        arrived(planes_in, PLANE - 1, sent3)

    @pl.when(jnp.logical_not(owner))
    def _():
        pltpu.make_async_copy(part, part, sent1).wait()


def per_device(prognostic_values, forcing_host_values, strength, level_height, pbl_height):
    hbm = pl.BlockSpec(memory_space=pltpu.HBM)
    smem = pl.BlockSpec(memory_space=pltpu.SMEM)
    vmem = pl.BlockSpec(memory_space=pltpu.VMEM)
    dma = pltpu.SemaphoreType.DMA
    return pl.pallas_call(
        kernel,
        out_shape=(
            jax.ShapeDtypeStruct((LEVELS, VARS, ROWS, COLS), bf16),
            jax.ShapeDtypeStruct((LEVELS, VARS), f32),
        ),
        in_specs=[hbm, hbm, smem, smem, hbm],
        out_specs=(vmem, vmem),
        scratch_shapes=[
            pltpu.VMEM((FIELDS, ROWS, COLS), f32),
            pltpu.VMEM((FIELDS, ROWS, COLS), bf16),
            pltpu.VMEM((ROWS, COLS), f32),
            pltpu.VMEM((LEVELS, ROWS, COLS), f32),
            pltpu.VMEM((COLS, 256), bf16),
            pltpu.VMEM((MODES, 512), bf16),
            pltpu.VMEM((ROWS, 128), bf16),
            pltpu.VMEM((128, COLS), bf16),
            pltpu.VMEM((GROUPS, 4, 8, 128), f32),
            pltpu.VMEM((PLANE, 8, 128), f32),
            pltpu.VMEM((PLANES, 8, 128), f32),
            pltpu.VMEM((GROUPS * 4, 8, 128), f32),
            dma((FIELDS,)), dma((FIELDS,)), dma(()),
            dma(()), dma(()), dma(()), dma(()), dma(()), dma((GROUPS,)),
        ],
        compiler_params=pltpu.CompilerParams(
            collective_id=0, has_side_effects=True, vmem_limit_bytes=40 * 1024 * 1024
        ),
    )(prognostic_values, forcing_host_values, strength, level_height, pbl_height)


def solution(mesh):
    return jax.shard_map(
        per_device,
        mesh=mesh,
        in_specs=(P(None, None, "gx", "gy"), P(None, None, "gx", "gy"), P(), P(), P("gx", "gy")),
        out_specs=(P(None, None, "gx", "gy"), P()),
        check_vma=False,
    )
```
